256 devices in a mesh: basis: 32 (over z, x_lo, core), band: 8 (over x_hi, y).
Axes of the slice: x: 4 (x_hi: 2, x_lo: 2; x = x_hi * 2 + x_lo), y: 4, z: 8, core: 2. Of those that a mesh axis runs over, the one named last changes fastest.
Arguments:
- matching: bfloat16 [162, 81920], P(None, 'basis'), may hold values from -6 to 6
- vectors: bfloat16 [81920, 16384], P('basis', 'band'), may hold values from -0.01953125 to 0.01953125
- weights: float32 [16384], P('band'), may hold values from 1.2207031e-05 to 0.00012207031
- gaunt_index: int32 [3, 4096], replicated, may hold values from 0 to 80
- gaunt_value: float32 [4096], replicated, may hold values from -4 to 4
Outputs:
- density_matrix: float32 [162, 162], replicated
- density: float32 [4, 81], replicated
The draws below stay inside these ranges and needn't reach their ends.
All inputs are finite; a program needn't handle non-finite values.
Results may differ from the reference program's by a relative error of at most 0.0003.
Values sent between devices are 32-bit elements; how exact they have to be, the bound alone decides.
A program may use at most 64 MiB of HBM per device.

```python
import math
import jax
import jax.numpy as jnp
from jax import lax

HARM = 81
CH = 162
NBASIS = 81920
BAND_DEV = 2048
NBANDS = 16384
NGAUNT = 4096


def touch_ends(values, key, smallest, high):
    spot = [jax.random.randint(jax.random.fold_in(key, axis), (), 0, length) for axis, length in enumerate(values.shape)]
    longest = values.shape.index(max(values.shape))
    next_to = spot[:longest] + [(spot[longest] + 1) % values.shape[longest]] + spot[longest + 1:]
    return values.at[tuple(spot)].set(smallest).at[tuple(next_to)].set(high)


def levels(rng, extent, split, smallest, largest):
    gain = 1.0
    for axis_at, shards_of in split:
        steps = jax.random.uniform(jax.random.fold_in(jax.random.fold_in(rng, 6), axis_at), (shards_of,), jnp.float32, smallest / len(split), largest / len(split))
        gain = gain * jnp.repeat(jnp.exp(steps), extent[axis_at] // shards_of).reshape((-1,) + (1,) * (len(extent) - 1 - axis_at))
    return gain


def centred(own_key, extent, scale, limit, split=(), kind=jnp.bfloat16):
    array = jax.random.normal(own_key, extent, jnp.float32) * scale
    if len(split) > 0:
        array = levels(own_key, extent, split, -0.22, 0.18) * array
    return jnp.clip(array, min=-limit, max=limit).astype(kind)


def setup_inputs(seed: int = 0) -> dict:
    key_of = jax.random.split(jax.random.key(seed), 6)
    return {
        "matching": centred(key_of[0], (CH, NBASIS), 1.0, 6.0, ((1, 32),)),
        "vectors": centred(key_of[1], (NBASIS, NBANDS), NBASIS ** -0.5, 0.01953125, ((0, 32), (1, 8))),
        "weights": jnp.clip(jnp.exp(math.log(0.00012207031) - 2.3025851 * jax.random.uniform(key_of[2], (NBANDS,), jnp.float32) ** levels(key_of[2], (NBANDS,), ((0, 8),), -0.2, 0.2)), 1.220703143189894e-05, 0.00012207031),
        "gaunt_index": touch_ends(jax.random.randint(key_of[3], (3, NGAUNT), 0, HARM), jax.random.fold_in(key_of[3], 1), 0, HARM - 1).astype(jnp.int32),
        "gaunt_value": centred(key_of[4], (NGAUNT,), 0.3, 4.0, (), jnp.float32),
    }


def reference(matching, vectors, weights, gaunt_index, gaunt_value):
    blocks = NBANDS // BAND_DEV
    left = matching.astype(jnp.float32)

    def one_block(index):
        start = (index * BAND_DEV).astype(jnp.int32)
        piece = lax.dynamic_slice_in_dim(vectors, start, BAND_DEV, 1).astype(jnp.float32)
        coeffs = jnp.dot(left, piece, precision=lax.Precision.HIGHEST, preferred_element_type=jnp.float32)
        scaled = coeffs * lax.dynamic_slice_in_dim(weights, start, BAND_DEV, 0)[None, :]
        return jnp.dot(scaled, coeffs.T, precision=lax.Precision.HIGHEST, preferred_element_type=jnp.float32)

    terms = lax.map(one_block, jnp.arange(blocks, dtype=jnp.int32))
    density_matrix = jnp.sum(terms, axis=0)
    blocked = density_matrix.reshape(2, HARM, 2, HARM)
    picked = blocked[:, gaunt_index[0], :, gaunt_index[1]]
    values = picked.reshape(NGAUNT, 4) * gaunt_value[:, None]
    density = jax.ops.segment_sum(values, gaunt_index[2], num_segments=HARM)
    return density_matrix, density.T
```

```python
import jax
import jax.numpy as jnp
from jax import lax
from jax.experimental import pallas as pl
from jax.experimental.pallas import tpu as pltpu
from jax.sharding import PartitionSpec as P

CH = 162
ROWS = 168
HALF = 88
SHIFT = 80
Z = 8
X = 4
Y = 4
LANES = 128
TILES = 32
OFFSETS = (4, 3, 5, 2, 6, 1, 7, 0)
PLANE = tuple((dx, dy) for dx in (2, 1, 3, 0) for dy in (2, 1, 3, 0))
MESH = pl.DeviceIdType.MESH
F32 = jnp.float32


def place(x, y, z, core):
    return {
        "basis": (z * 2 + lax.rem(x, 2)) * 2 + core,
        "band": lax.div(x, 2) * Y + y,
    }


def kernel(
    a_hbm, v_hbm, w_ref, out_ref,
    a_buf, v_buf, part, core_in, pair, x_in, z_out, z_in, full, terms, plane_in,
    own_tile, line_in, tiles,
    a_sem, v_sem, core_s, core_r, x_s, x_r, z_s, z_r, full_s, full_r,
    plane_s, plane_r, line_s, line_r, all_s, all_r,
):
    basis, band = lax.axis_index("basis"), lax.axis_index("band")
    z, xl, core = lax.div(basis, 4), lax.rem(lax.div(basis, 2), 2), lax.rem(basis, 2)
    x, y = lax.div(band, Y) * 2 + xl, lax.rem(band, Y)
    other = 1 - core

    a_copy = pltpu.make_async_copy(a_hbm, a_buf, a_sem)
    a_copy.start()
    targets = [lax.rem(z + off, Z) for off in OFFSETS]
    v_copies = []
    for s in range(Z):
        columns = pl.ds(pl.multiple_of(targets[s] * 256, 256), 256)
        v_copies.append(pltpu.make_async_copy(v_hbm.at[:, columns], v_buf.at[s], v_sem.at[s]))
        v_copies[s].start()

    plane = [
        (place(lax.rem(x + dx, X), lax.rem(y + dy, Y), z, c), dx, dy, flip)
        for dx, dy in PLANE
        for flip, c in ((0, core), (1, other))
        if (dx, dy, flip) != (0, 0, 0)
    ]
    line = [place(x, y, lax.rem(z + dz, Z), core) for dz in range(1, Z)]
    barrier = pltpu.get_barrier_semaphore()
    for device, *_ in plane:
        pl.semaphore_signal(barrier, inc=1, device_id=device, device_id_type=MESH)
    for device in line:
        pl.semaphore_signal(barrier, inc=1, device_id=device, device_id_type=MESH)

    for s in range(Z):
        for h in range(2):
            part[s, h, SHIFT * 2 : ROWS, :] = jnp.zeros((ROWS - SHIFT * 2, LANES), F32)
    full[ROWS:256, :] = jnp.zeros((256 - ROWS, LANES), F32)
    terms[26:TILES] = jnp.zeros((TILES - 26, 8, LANES), F32)

    core_peer = place(x, y, z, other)
    x_peer = place(x + 1 - 2 * xl, y, z, core)

    def remote(src, dst, send, recv, device):
        return pltpu.make_async_remote_copy(
            src_ref=src, dst_ref=dst, send_sem=send, recv_sem=recv,
            device_id=device, device_id_type=MESH,
        )

    mine = pl.ds(pl.multiple_of(SHIFT * core, 8), HALF)
    theirs = pl.ds(pl.multiple_of(SHIFT * other, 8), HALF)
    core_copies, x_copies, z_copies = [], [], []

    def multiply(s):
        v_copies[s].wait()
        product = jnp.dot(a_buf[...], v_buf[s], preferred_element_type=F32)
        part[s, 0, 0:CH, :] = product[:, :LANES]
        part[s, 1, 0:CH, :] = product[:, LANES:]

    def to_core(s):
        copy = remote(part.at[s, :, theirs, :], core_in.at[s], core_s.at[s], core_r.at[s], core_peer)
        copy.start()
        core_copies.append(copy)

    def to_x(s):
        core_copies[s].wait_recv()
        pair[s] = part[s, :, mine, :] + core_in[s]
        copy = remote(pair.at[s, 1 - xl], x_in.at[s], x_s.at[s], x_r.at[s], x_peer)
        copy.start()
        x_copies.append(copy)

    def to_z(s):
        x_copies[s].wait_recv()
        total = pair[s, xl] + x_in[s]
        z_out[s] = total
        if OFFSETS[s]:
            copy = remote(
                z_out.at[s], z_in.at[s], z_s.at[s], z_r.at[s], place(x, y, targets[s], core)
            )
            copy.start()
            z_copies.append(copy)

    a_copy.wait()
    multiply(0)
    pl.semaphore_wait(barrier, len(plane) + len(line))
    to_core(0)
    for s in range(1, Z):
        multiply(s)
        to_core(s)
        if s >= 3:
            to_x(s - 3)
    for s in range(Z - 3, Z):
        to_x(s)
    for s in range(Z):
        to_z(s)
    total = z_out[Z - 1]
    for s in range(Z - 1):
        z_copies[s].wait_recv()
        total = total + z_in[s]

    full[mine, :] = total
    sent = pl.ds(pl.multiple_of(HALF * core, 8), SHIFT)
    full_copy = remote(full.at[sent, :], full.at[sent, :], full_s, full_r, core_peer)
    full_copy.start()
    own_weights = w_ref[pl.ds(z * 2 + xl, 1), :]
    full_copy.wait()

    coeffs = full[0:ROWS, :]
    scaled = coeffs * own_weights
    contract = (((1,), (1,)), ((), ()))
    upper = lax.dot_general(
        scaled, full[0:LANES, :], contract,
        precision=lax.Precision.HIGHEST, preferred_element_type=F32,
    )
    corner = lax.dot_general(
        scaled[LANES:ROWS], full[LANES:256, :], contract,
        precision=lax.Precision.HIGHEST, preferred_element_type=F32,
    )
    terms[0:21] = upper.reshape(21, 8, LANES)
    terms[21:26] = corner.reshape(5, 8, LANES)

    plane_copies = []
    for dx, dy in PLANE[:-1]:
        j = len(plane_copies)
        xt, yt = lax.rem(x + dx, X), lax.rem(y + dy, Y)
        copy = remote(
            terms.at[(xt * Y + yt) * 2 + core], plane_in.at[j], plane_s.at[j], plane_r.at[j],
            place(xt, yt, z, core),
        )
        copy.start()
        plane_copies.append(copy)
    own = (x * Y + y) * 2 + core
    tile = terms[own]
    for j, copy in reversed(list(enumerate(plane_copies))):
        copy.wait_recv()
        tile = tile + plane_in[j]

    own_tile[...] = tile
    line_copies = []
    for j in (3, 2, 4, 1, 5, 0, 6):
        copy = remote(own_tile, line_in.at[j], line_s.at[j], line_r.at[j], line[j])
        copy.start()
        line_copies.append((j, copy))
    for j, copy in reversed(line_copies):
        copy.wait_recv()
        tile = tile + line_in[j]

    tiles[own] = tile
    all_copies = []
    for device, *_ in plane:
        j = len(all_copies)
        copy = remote(tiles.at[own], tiles.at[own], all_s.at[j], all_r.at[j], device)
        copy.start()
        all_copies.append(copy)
    for j, (_, dx, dy, flip) in enumerate(plane):
        xs, ys = lax.rem(x + X - dx, X), lax.rem(y + Y - dy, Y)
        cs = core if flip == 0 else other
        slot = tiles.at[(xs * Y + ys) * 2 + cs]
        remote(slot, slot, all_s.at[j], all_r.at[j], core_peer).wait_recv()
    for copy in core_copies + x_copies + z_copies + plane_copies + all_copies:
        copy.wait_send()
    for _, copy in line_copies:
        copy.wait_send()
    out_ref[...] = tiles[...]


def reduced_tiles(matching, vectors, weights):
    dma = pltpu.SemaphoreType.DMA
    depth = matching.shape[1]
    return pl.pallas_call(
        kernel,
        out_shape=jax.ShapeDtypeStruct((TILES, 8, LANES), F32),
        in_specs=[
            pl.BlockSpec(memory_space=pl.ANY),
            pl.BlockSpec(memory_space=pl.ANY),
            pl.BlockSpec(memory_space=pltpu.VMEM),
        ],
        out_specs=pl.BlockSpec(memory_space=pltpu.VMEM),
        scratch_shapes=[
            pltpu.VMEM((CH, depth), jnp.bfloat16),
            pltpu.VMEM((Z, depth, 256), jnp.bfloat16),
            pltpu.VMEM((Z, 2, ROWS, LANES), F32),
            pltpu.VMEM((Z, 2, HALF, LANES), F32),
            pltpu.VMEM((Z, 2, HALF, LANES), F32),
            pltpu.VMEM((Z, HALF, LANES), F32),
            pltpu.VMEM((Z, HALF, LANES), F32),
            pltpu.VMEM((Z - 1, HALF, LANES), F32),
            pltpu.VMEM((256, LANES), F32),
            pltpu.VMEM((TILES, 8, LANES), F32),
            pltpu.VMEM((15, 8, LANES), F32),
            pltpu.VMEM((8, LANES), F32),
            pltpu.VMEM((7, 8, LANES), F32),
            pltpu.VMEM((TILES, 8, LANES), F32),
            dma, dma((Z,)),
            dma((Z,)), dma((Z,)), dma((Z,)), dma((Z,)), dma((Z - 1,)), dma((Z - 1,)), dma, dma,
            dma((15,)), dma((15,)), dma((7,)), dma((7,)), dma((31,)), dma((31,)),
        ],
        compiler_params=pltpu.CompilerParams(
            collective_id=0, has_side_effects=True, vmem_limit_bytes=40 * 1024 * 1024
        ),
        name="reduced_tiles",
    )(matching, vectors, weights.reshape(-1, LANES))


def gaunt_density(density_matrix, gaunt_index, gaunt_value):
    harmonics = density_matrix.shape[0] // 2
    codes = jnp.arange(harmonics, dtype=jnp.int32)[:, None]
    first_table = (gaunt_index[0][None, :] == codes).astype(F32)
    second_table = (gaunt_index[1][None, :] == codes).astype(F32)
    target_table = (gaunt_index[2][None, :] == codes).astype(F32)
    collected = []
    for radial in range(2):
        for other in range(2):
            block = density_matrix[
                radial * harmonics : (radial + 1) * harmonics,
                other * harmonics : (other + 1) * harmonics,
            ]
            spread = jnp.dot(
                block, second_table, precision=lax.Precision.HIGHEST, preferred_element_type=F32
            )
            collected.append(jnp.sum(spread * first_table, axis=0) * gaunt_value)
    return lax.dot_general(
        jnp.stack(collected), target_table, (((1,), (1,)), ((), ())),
        precision=lax.Precision.HIGHEST, preferred_element_type=F32,
    )


def body(matching, vectors, weights, gaunt_index, gaunt_value):
    tiles = reduced_tiles(matching, vectors, weights)
    left = tiles[:21].reshape(ROWS, LANES)[:CH]
    corner = tiles[21:26].reshape(40, LANES)[: CH - LANES, : CH - LANES]
    right = jnp.concatenate([left[LANES:].T, corner], axis=0)
    density_matrix = jnp.concatenate([left, right], axis=1)
    return density_matrix, gaunt_density(density_matrix, gaunt_index, gaunt_value)


def solution(mesh):
    return jax.shard_map(
        body,
        mesh=mesh,
        in_specs=(P(None, "basis"), P("basis", "band"), P("band"), P(), P()),
        out_specs=(P(), P()),
        check_vma=False,
    )
```

```python
import jax
import jax.numpy as jnp
from jax import lax
from jax.experimental import pallas as pl
from jax.experimental.pallas import tpu as pltpu
from jax.sharding import PartitionSpec as P

CH = 162
ROWS = 168
HALF = 88
SHIFT = 80
Z = 8
X = 4
Y = 4
LANES = 128
TILES = 32
HARM = 81
ENTRIES = 4096
CHUNK = 512
OFFSETS = (4, 3, 5, 2, 6, 1, 7, 0)
PLANE = tuple((dx, dy) for dx in (2, 1, 3, 0) for dy in (2, 1, 3, 0))
MESH = pl.DeviceIdType.MESH
F32 = jnp.float32
BF16 = jnp.bfloat16


def place(x, y, z, core):
    return {
        "basis": (z * 2 + lax.rem(x, 2)) * 2 + core,
        "band": lax.div(x, 2) * Y + y,
    }


def halves(value):
    high = value.astype(BF16)
    return high, (value - high.astype(F32)).astype(BF16)


def harmonic_of(channel):
    folded = jnp.where(channel >= HARM, channel - HARM, channel)
    return jnp.where(channel < CH, folded, -1)


def kernel(
    a_hbm, v_hbm, w_hbm, index_hbm, value_hbm, matrix_ref, density_ref,
    a_buf, v_buf, part, core_in, pair, x_in, z_out, z_in, full, terms, plane_in,
    own_tile, line_in, tiles, w_buf, index_buf, value_buf, hot, target_hot, factor, sums,
    a_sem, v_sem, table_sem, core_s, core_r, x_s, x_r, z_s, z_r, full_s, full_r,
    plane_s, plane_r, line_s, line_r, all_s, all_r, sum_s, sum_r,
):
    basis, band = lax.axis_index("basis"), lax.axis_index("band")
    z, xl, core = lax.div(basis, 4), lax.rem(lax.div(basis, 2), 2), lax.rem(basis, 2)
    x, y = lax.div(band, Y) * 2 + xl, lax.rem(band, Y)
    other = 1 - core
    own = (x * Y + y) * 2 + core

    a_copy = pltpu.make_async_copy(a_hbm, a_buf, a_sem)
    a_copy.start()
    targets = [lax.rem(z + off, Z) for off in OFFSETS]
    v_copies = []
    for s in range(Z):
        columns = pl.ds(pl.multiple_of(targets[s] * 256, 256), 256)
        place_in = v_buf.at[s // 2, :, (s % 2) * 256 : (s % 2) * 256 + 256]
        v_copies.append(pltpu.make_async_copy(v_hbm.at[:, columns], place_in, v_sem.at[s]))
    for s in range(4):
        v_copies[s].start()
    table_copies = [
        pltpu.make_async_copy(w_hbm, w_buf, table_sem.at[0]),
        pltpu.make_async_copy(index_hbm, index_buf, table_sem.at[1]),
        pltpu.make_async_copy(value_hbm, value_buf, table_sem.at[2]),
    ]

    plane = [
        (place(lax.rem(x + dx, X), lax.rem(y + dy, Y), z, c), dx, dy, flip)
        for dx, dy in PLANE
        for flip, c in ((0, core), (1, other))
        if (dx, dy, flip) != (0, 0, 0)
    ]
    line = [place(x, y, lax.rem(z + dz, Z), core) for dz in range(1, Z)]
    barrier = pltpu.get_barrier_semaphore()
    for device, *_ in plane:
        pl.semaphore_signal(barrier, inc=1, device_id=device, device_id_type=MESH)
    for device in line:
        pl.semaphore_signal(barrier, inc=1, device_id=device, device_id_type=MESH)

    for s in range(Z):
        for h in range(2):
            part[s, h, SHIFT * 2 : ROWS, :] = jnp.zeros((ROWS - SHIFT * 2, LANES), F32)
    full[ROWS:256, :] = jnp.zeros((256 - ROWS, LANES), F32)
    terms[26:TILES] = jnp.zeros((TILES - 26, 8, LANES), F32)

    core_peer = place(x, y, z, other)
    x_peer = place(x + 1 - 2 * xl, y, z, core)

    def remote(src, dst, send, recv, device):
        return pltpu.make_async_remote_copy(
            src_ref=src, dst_ref=dst, send_sem=send, recv_sem=recv,
            device_id=device, device_id_type=MESH,
        )

    mine = pl.ds(pl.multiple_of(SHIFT * core, 8), HALF)
    theirs = pl.ds(pl.multiple_of(SHIFT * other, 8), HALF)
    core_copies, x_copies, z_copies = [], [], []
    plane_copies, line_copies, all_copies = [], [], []

    def multiply(c):
        v_copies[2 * c].wait()
        v_copies[2 * c + 1].wait()
        if c + 2 < Z // 2:
            v_copies[2 * c + 4].start()
            v_copies[2 * c + 5].start()
        product = jnp.dot(a_buf[...], v_buf[c], preferred_element_type=F32)
        for s in (2 * c, 2 * c + 1):
            for h in range(2):
                at = (s % 2) * 256 + h * LANES
                part[s, h, 0:CH, :] = product[:, at : at + LANES]

    def to_core(s):
        copy = remote(part.at[s, :, theirs, :], core_in.at[s], core_s.at[s], core_r.at[s], core_peer)
        copy.start()
        core_copies.append(copy)

    def to_x(s):
        core_copies[s].wait_recv()
        pair[s] = part[s, :, mine, :] + core_in[s]
        copy = remote(pair.at[s, 1 - xl], x_in.at[s], x_s.at[s], x_r.at[s], x_peer)
        copy.start()
        x_copies.append(copy)

    def to_z(s):
        x_copies[s].wait_recv()
        z_out[s] = pair[s, xl] + x_in[s]
        if OFFSETS[s]:
            copy = remote(
                z_out.at[s], z_in.at[s], z_s.at[s], z_r.at[s], place(x, y, targets[s], core)
            )
            copy.start()
            z_copies.append(copy)

    first_row = own * 8 - jnp.where(own < 21, 0, 40)
    first_column = jnp.where(own < 21, 0, LANES)
    mirrored = jnp.where(jnp.logical_and(own >= 16, own < 21), 1.0, 0.0).astype(F32)
    row_channel = first_row + lax.broadcasted_iota(jnp.int32, (8, 1), 0)

    def tables(n):
        at = slice(n * CHUNK, (n + 1) * CHUNK)
        first, second = index_buf[0:1, at], index_buf[1:2, at]
        target, value = index_buf[2:3, at], value_buf[0:1, at]
        column = harmonic_of(first_column + lax.broadcasted_iota(jnp.int32, (LANES, 1), 0))
        hot[0:LANES, at] = jnp.where(column == second, 1.0, 0.0).astype(BF16)
        hot[LANES : 2 * LANES, at] = jnp.where(column == first, 1.0, 0.0).astype(BF16)
        code = lax.broadcasted_iota(jnp.int32, (LANES, 1), 0)
        target_hot[:, at] = jnp.where(code == target, 1.0, 0.0).astype(BF16)
        row = harmonic_of(row_channel)
        factor[0:8, at] = jnp.where(row == first, value, 0.0)
        factor[8:16, at] = jnp.where(row == second, value, 0.0) * mirrored

    def contracted(tile):
        lane = first_column + lax.broadcasted_iota(jnp.int32, (8, LANES), 1)
        none = jnp.zeros((8, LANES), F32)
        lows = jnp.where(lane < HARM, tile, 0.0)
        highs = jnp.where(lane < HARM, 0.0, tile)
        wide = jnp.concatenate(
            [
                jnp.concatenate([lows, highs, none, none], axis=0),
                jnp.concatenate([none, none, lows, highs], axis=0),
            ],
            axis=1,
        )
        both = jnp.concatenate(halves(wide), axis=0)
        total = jnp.zeros((8, LANES), F32)
        for n in range(ENTRIES // 1024):
            at = slice(n * 1024, (n + 1) * 1024)
            spread = jnp.dot(both, hot[:, at], preferred_element_type=F32)
            spread = spread[0:32] + spread[32:64]
            direct, mirror = factor[0:8, at], factor[8:16, at]
            low, high = spread[0:8] * direct, spread[8:16] * direct
            mirror_low, mirror_high = spread[16:24] * mirror, spread[24:32] * mirror
            upper = row_channel >= HARM
            rows = [
                jnp.where(upper, 0.0, low),
                jnp.where(upper, 0.0, high) + mirror_low,
                jnp.where(upper, low, 0.0),
                jnp.where(upper, high, 0.0) + mirror_high,
            ]
            values = jnp.concatenate([jnp.sum(row, axis=0, keepdims=True) for row in rows], axis=0)
            total = total + lax.dot_general(
                jnp.concatenate(halves(values), axis=0), target_hot[:, at],
                (((1,), (1,)), ((), ())), preferred_element_type=F32,
            )
        return total[0:4] + total[4:8]

    def finish():
        for copy in core_copies + x_copies + z_copies + plane_copies + line_copies + all_copies:
            copy.wait_send()

    a_copy.wait()
    multiply(0)
    pl.semaphore_wait(barrier, len(plane) + len(line))
    to_core(0)
    to_core(1)
    for copy in table_copies:
        copy.start()
    multiply(1)
    to_core(2)
    to_core(3)
    to_x(0)
    to_x(1)
    multiply(2)
    to_core(4)
    to_core(5)
    to_x(2)
    to_x(3)
    multiply(3)
    to_core(6)
    to_core(7)
    to_x(4)
    to_x(5)
    for copy in table_copies:
        copy.wait()
    to_x(6)
    to_x(7)
    for s in range(Z):
        tables(s)
        to_z(s)
    total = z_out[Z - 1]
    for s in range(Z - 1):
        z_copies[s].wait_recv()
        total = total + z_in[s]

    full[mine, :] = total
    sent = pl.ds(pl.multiple_of(HALF * core, 8), SHIFT)
    full_copy = remote(full.at[sent, :], full.at[sent, :], full_s, full_r, core_peer)
    full_copy.start()
    own_weights = w_buf[pl.ds(z * 2 + xl, 1), :]
    full_copy.wait()

    coeffs = full[...]
    high, low = halves(coeffs)
    scaled_high, scaled_low = halves(coeffs[0:ROWS] * own_weights)
    product = lax.dot_general(
        jnp.concatenate([scaled_high, scaled_low, scaled_high], axis=1),
        jnp.concatenate([high, high, low], axis=1),
        (((1,), (1,)), ((), ())), preferred_element_type=F32,
    )
    terms[0:21] = product[:, 0:LANES].reshape(21, 8, LANES)
    terms[21:26] = product[LANES:ROWS, LANES:256].reshape(5, 8, LANES)

    for dx, dy in PLANE[:-1]:
        j = len(plane_copies)
        xt, yt = lax.rem(x + dx, X), lax.rem(y + dy, Y)
        copy = remote(
            terms.at[(xt * Y + yt) * 2 + core], plane_in.at[j], plane_s.at[j], plane_r.at[j],
            place(xt, yt, z, core),
        )
        copy.start()
        plane_copies.append(copy)
    tile = terms[own]
    for j, copy in reversed(list(enumerate(plane_copies))):
        copy.wait_recv()
        tile = tile + plane_in[j]

    own_tile[...] = tile
    for j in (3, 2, 4, 1, 5, 0, 6):
        copy = remote(own_tile, line_in.at[j], line_s.at[j], line_r.at[j], line[j])
        copy.start()
        line_copies.append(copy)
    for j, copy in reversed(list(zip((3, 2, 4, 1, 5, 0, 6), line_copies))):
        copy.wait_recv()
        tile = tile + line_in[j]

    def to_all(buffer, send, recv):
        for j, (device, *_) in enumerate(plane):
            copy = remote(buffer.at[own], buffer.at[own], send.at[j], recv.at[j], device)
            copy.start()
            all_copies.append(copy)

    def from_all(buffer, send, recv):
        for j, (_, dx, dy, flip) in enumerate(plane):
            xs, ys = lax.rem(x + X - dx, X), lax.rem(y + Y - dy, Y)
            slot = buffer.at[(xs * Y + ys) * 2 + (core if flip == 0 else other)]
            remote(slot, slot, send.at[j], recv.at[j], core_peer).wait_recv()

    tiles[own] = tile
    to_all(tiles, all_s, all_r)
    sums[own] = contracted(tile)
    to_all(sums, sum_s, sum_r)
    from_all(tiles, all_s, all_r)
    left = tiles[0:21].reshape(ROWS, LANES)
    matrix_ref[:, 0:LANES] = left[0:CH]
    matrix_ref[0:LANES, LANES:CH] = left[LANES:ROWS].T[:, 0 : CH - LANES]
    matrix_ref[LANES:CH, LANES:CH] = tiles[21:26].reshape(40, LANES)[0 : CH - LANES, 0 : CH - LANES]
    from_all(sums, sum_s, sum_r)
    density_ref[...] = jnp.sum(sums[...], axis=0)[:, 0:HARM]
    finish()


def body(matching, vectors, weights, gaunt_index, gaunt_value):
    dma = pltpu.SemaphoreType.DMA
    depth = matching.shape[1]
    return pl.pallas_call(
        kernel,
        out_shape=(
            jax.ShapeDtypeStruct((CH, CH), F32),
            jax.ShapeDtypeStruct((4, HARM), F32),
        ),
        in_specs=[pl.BlockSpec(memory_space=pl.ANY)] * 5,
        out_specs=(
            pl.BlockSpec(memory_space=pltpu.VMEM),
            pl.BlockSpec(memory_space=pltpu.VMEM),
        ),
        scratch_shapes=[
            pltpu.VMEM((CH, depth), BF16),
            pltpu.VMEM((Z // 2, depth, 512), BF16),
            pltpu.VMEM((Z, 2, ROWS, LANES), F32),
            pltpu.VMEM((Z, 2, HALF, LANES), F32),
            pltpu.VMEM((Z, 2, HALF, LANES), F32),
            pltpu.VMEM((Z, HALF, LANES), F32),
            pltpu.VMEM((Z, HALF, LANES), F32),
            pltpu.VMEM((Z - 1, HALF, LANES), F32),
            pltpu.VMEM((256, LANES), F32),
            pltpu.VMEM((TILES, 8, LANES), F32),
            pltpu.VMEM((15, 8, LANES), F32),
            pltpu.VMEM((8, LANES), F32),
            pltpu.VMEM((7, 8, LANES), F32),
            pltpu.VMEM((TILES, 8, LANES), F32),
            pltpu.VMEM((16, LANES), F32),
            pltpu.VMEM((3, ENTRIES), jnp.int32),
            pltpu.VMEM((1, ENTRIES), F32),
            pltpu.VMEM((2 * LANES, ENTRIES), BF16),
            pltpu.VMEM((LANES, ENTRIES), BF16),
            pltpu.VMEM((16, ENTRIES), F32),
            pltpu.VMEM((TILES, 4, LANES), F32),
            dma, dma((Z,)), dma((3,)),
            dma((Z,)), dma((Z,)), dma((Z,)), dma((Z,)), dma((Z - 1,)), dma((Z - 1,)), dma, dma,
            dma((15,)), dma((15,)), dma((7,)), dma((7,)),
            dma((31,)), dma((31,)), dma((31,)), dma((31,)),
        ],
        compiler_params=pltpu.CompilerParams(
            collective_id=0, has_side_effects=True, vmem_limit_bytes=67_043_328
        ),
        name="muffin_tin",
    )(matching, vectors, weights.reshape(-1, LANES), gaunt_index, gaunt_value.reshape(1, -1))


def solution(mesh):
    return jax.shard_map(
        body,
        mesh=mesh,
        in_specs=(P(None, "basis"), P("basis", "band"), P("band"), P(), P()),
        out_specs=(P(), P()),
        check_vma=False,
    )
```

```python
import jax
import jax.numpy as jnp
from jax import lax
from jax.experimental import pallas as pl
from jax.experimental.pallas import tpu as pltpu
from jax.sharding import PartitionSpec as P

CH = 162
ROWS = 168
HALF = 88
SHIFT = 80
Z = 8
X = 4
Y = 4
LANES = 128
TILES = 32
HARM = 81
ENTRIES = 4096
CHUNK = 512
GROUPS = ((4,), (3, 5), (1, 7), (2, 6), (0,))
VIA = 48
PLANE = tuple((dx, dy) for dx in (2, 1, 3, 0) for dy in (2, 1, 3, 0))
MESH = pl.DeviceIdType.MESH
F32 = jnp.float32
BF16 = jnp.bfloat16


def place(x, y, z, core):
    return {
        "basis": (z * 2 + lax.rem(x, 2)) * 2 + core,
        "band": lax.div(x, 2) * Y + y,
    }


def halves(value):
    high = value.astype(BF16)
    return high, (value - high.astype(F32)).astype(BF16)


def harmonic_of(channel):
    folded = jnp.where(channel >= HARM, channel - HARM, channel)
    return jnp.where(channel < CH, folded, -1)


def kernel(
    a_hbm, v_hbm, w_hbm, index_hbm, value_hbm, matrix_ref, density_ref,
    a_buf, v_wide, v_slim, part, core_in, pair, x_in, z_out, far, thirds, nexts, seconds,
    full, terms, plane_in,
    own_tile, line_in, tiles, w_buf, index_buf, value_buf, hot, target_hot, factor, sums,
    a_sem, v_sem, table_sem, core_s, core_r, x_s, x_r, z_s, z_r, full_s, full_r,
    plane_s, plane_r, line_s, line_r, all_s, all_r, sum_s, sum_r,
):
    basis, band = lax.axis_index("basis"), lax.axis_index("band")
    z, xl, core = lax.div(basis, 4), lax.rem(lax.div(basis, 2), 2), lax.rem(basis, 2)
    x, y = lax.div(band, Y) * 2 + xl, lax.rem(band, Y)
    other = 1 - core
    own = (x * Y + y) * 2 + core

    a_copy = pltpu.make_async_copy(a_hbm, a_buf, a_sem)
    a_copy.start()
    targets = [lax.rem(z + off, Z) for off in range(Z)]
    v_blocks = (v_slim.at[0], v_wide.at[0], v_wide.at[1], v_wide.at[2], v_slim.at[1])
    v_copies = []
    for group, block in zip(GROUPS, v_blocks):
        copies = []
        for h, off in enumerate(group):
            columns = pl.ds(pl.multiple_of(targets[off] * 256, 256), 256)
            copies.append(
                pltpu.make_async_copy(
                    v_hbm.at[:, columns], block.at[:, h * 256 : h * 256 + 256], v_sem.at[off]
                )
            )
        v_copies.append(copies)
    for copy in v_copies[0] + v_copies[1]:
        copy.start()
    table_copies = [
        pltpu.make_async_copy(w_hbm, w_buf, table_sem.at[0]),
        pltpu.make_async_copy(index_hbm, index_buf, table_sem.at[1]),
        pltpu.make_async_copy(value_hbm, value_buf, table_sem.at[2]),
    ]

    plane = [
        (place(lax.rem(x + dx, X), lax.rem(y + dy, Y), z, c), dx, dy, flip)
        for dx, dy in PLANE
        for flip, c in ((0, core), (1, other))
        if (dx, dy, flip) != (0, 0, 0)
    ]
    line = [place(x, y, lax.rem(z + dz, Z), core) for dz in range(1, Z)]
    barrier = pltpu.get_barrier_semaphore()
    for device, *_ in plane:
        pl.semaphore_signal(barrier, inc=1, device_id=device, device_id_type=MESH)
    for device in line:
        pl.semaphore_signal(barrier, inc=1, device_id=device, device_id_type=MESH)

    for s in range(Z):
        for h in range(2):
            part[s, h, SHIFT * 2 : ROWS, :] = jnp.zeros((ROWS - SHIFT * 2, LANES), F32)
    full[ROWS:256, :] = jnp.zeros((256 - ROWS, LANES), F32)
    terms[26:TILES] = jnp.zeros((TILES - 26, 8, LANES), F32)

    core_peer = place(x, y, z, other)
    x_peer = place(x + 1 - 2 * xl, y, z, core)

    def remote(src, dst, send, recv, device):
        return pltpu.make_async_remote_copy(
            src_ref=src, dst_ref=dst, send_sem=send, recv_sem=recv,
            device_id=device, device_id_type=MESH,
        )

    mine = pl.ds(pl.multiple_of(SHIFT * core, 8), HALF)
    theirs = pl.ds(pl.multiple_of(SHIFT * other, 8), HALF)
    core_copies, x_copies, z_copies = {}, {}, {}
    plane_copies, line_copies, all_copies = [], [], []

    def multiply(c):
        for copy in v_copies[c]:
            copy.wait()
        if c + 2 < len(GROUPS):
            for copy in v_copies[c + 2]:
                copy.start()
        product = jnp.dot(a_buf[...], v_blocks[c][...], preferred_element_type=F32)
        for g, off in enumerate(GROUPS[c]):
            for h in range(2):
                at = g * 256 + h * LANES
                part[off, h, 0:CH, :] = product[:, at : at + LANES]

    def to_core(off):
        core_copies[off] = remote(
            part.at[off, :, theirs, :], core_in.at[off], core_s.at[off], core_r.at[off], core_peer
        )
        core_copies[off].start()

    def of_core(off):
        core_copies[off].wait_recv()
        return part[off, :, mine, :] + core_in[off]

    def to_x(off, value):
        pair[off] = value
        x_copies[off] = remote(
            pair.at[off, 1 - xl], x_in.at[off], x_s.at[off], x_r.at[off], x_peer
        )
        x_copies[off].start()

    def of_x(off):
        x_copies[off].wait_recv()
        return pair[off, xl] + x_in[off]

    def to_z(key, src, dst, step):
        z_copies[key] = remote(
            src, dst, z_s.at[len(z_copies)], z_r.at[len(z_copies)], place(x, y, targets[step], core)
        )
        z_copies[key].start()

    def to_far():
        z_out[4] = of_x(4)
        to_z("up4", z_out.at[4, 0:VIA], far.at[0:VIA], 2)
        to_z("down4", z_out.at[4, VIA:HALF], far.at[VIA:HALF], 6)

    def to_third(off):
        z_out[off] = of_x(off)
        to_z(off, z_out.at[off], thirds.at[off // 4], 1 if off == 3 else 7)

    def to_next(off):
        pair[off] = of_core(off)
        to_z(off, pair.at[off], nexts.at[off // 4], off)

    def to_second(off):
        value = of_x(off)
        if off == 2:
            z_copies["up4"].wait_recv()
            z_copies[3].wait_recv()
            value = value + thirds[0]
            z_out[off, 0:VIA] = value[0:VIA] + far[0:VIA]
            z_out[off, VIA:HALF] = value[VIA:HALF]
        else:
            z_copies["down4"].wait_recv()
            z_copies[5].wait_recv()
            value = value + thirds[1]
            z_out[off, 0:VIA] = value[0:VIA]
            z_out[off, VIA:HALF] = value[VIA:HALF] + far[VIA:HALF]
        to_z(off, z_out.at[off], seconds.at[off // 4], off)

    first_row = own * 8 - jnp.where(own < 21, 0, 40)
    first_column = jnp.where(own < 21, 0, LANES)
    mirrored = jnp.where(jnp.logical_and(own >= 16, own < 21), 1.0, 0.0).astype(F32)
    row_channel = first_row + lax.broadcasted_iota(jnp.int32, (8, 1), 0)

    def tables(n):
        at = slice(n * CHUNK, (n + 1) * CHUNK)
        first, second = index_buf[0:1, at], index_buf[1:2, at]
        target, value = index_buf[2:3, at], value_buf[0:1, at]
        column = harmonic_of(first_column + lax.broadcasted_iota(jnp.int32, (LANES, 1), 0))
        hot[0:LANES, at] = jnp.where(column == second, 1.0, 0.0).astype(BF16)
        hot[LANES : 2 * LANES, at] = jnp.where(column == first, 1.0, 0.0).astype(BF16)
        code = lax.broadcasted_iota(jnp.int32, (LANES, 1), 0)
        target_hot[:, at] = jnp.where(code == target, 1.0, 0.0).astype(BF16)
        row = harmonic_of(row_channel)
        factor[0:8, at] = jnp.where(row == first, value, 0.0)
        factor[8:16, at] = jnp.where(row == second, value, 0.0) * mirrored

    def contracted(tile):
        lane = first_column + lax.broadcasted_iota(jnp.int32, (8, LANES), 1)
        none = jnp.zeros((8, LANES), F32)
        lows = jnp.where(lane < HARM, tile, 0.0)
        highs = jnp.where(lane < HARM, 0.0, tile)
        wide = jnp.concatenate(
            [
                jnp.concatenate([lows, highs, none, none], axis=0),
                jnp.concatenate([none, none, lows, highs], axis=0),
            ],
            axis=1,
        )
        both = jnp.concatenate(halves(wide), axis=0)
        total = jnp.zeros((8, LANES), F32)
        for n in range(ENTRIES // 1024):
            at = slice(n * 1024, (n + 1) * 1024)
            spread = jnp.dot(both, hot[:, at], preferred_element_type=F32)
            spread = spread[0:32] + spread[32:64]
            direct, mirror = factor[0:8, at], factor[8:16, at]
            low, high = spread[0:8] * direct, spread[8:16] * direct
            mirror_low, mirror_high = spread[16:24] * mirror, spread[24:32] * mirror
            upper = row_channel >= HARM
            rows = [
                jnp.where(upper, 0.0, low),
                jnp.where(upper, 0.0, high) + mirror_low,
                jnp.where(upper, low, 0.0),
                jnp.where(upper, high, 0.0) + mirror_high,
            ]
            values = jnp.concatenate([jnp.sum(row, axis=0, keepdims=True) for row in rows], axis=0)
            total = total + lax.dot_general(
                jnp.concatenate(halves(values), axis=0), target_hot[:, at],
                (((1,), (1,)), ((), ())), preferred_element_type=F32,
            )
        return total[0:4] + total[4:8]

    def finish():
        for copies in (core_copies, x_copies, z_copies):
            for copy in copies.values():
                copy.wait_send()
        for copy in plane_copies + line_copies + all_copies:
            copy.wait_send()

    a_copy.wait()
    multiply(0)
    pl.semaphore_wait(barrier, len(plane) + len(line))
    to_core(4)
    for copy in table_copies:
        copy.start()
    multiply(1)
    to_core(3)
    to_core(5)
    to_x(4, of_core(4))
    multiply(2)
    to_core(1)
    to_core(7)
    to_x(3, of_core(3))
    to_x(5, of_core(5))
    multiply(3)
    to_core(2)
    to_core(6)
    to_next(1)
    to_next(7)
    multiply(4)
    to_core(0)
    to_far()
    to_x(2, of_core(2))
    to_x(6, of_core(6))
    to_third(3)
    to_third(5)
    own_sum = of_core(0)
    for copy in table_copies:
        copy.wait()
    for n in range(2):
        tables(n)
    z_copies[1].wait_recv()
    z_copies[7].wait_recv()
    to_x(0, own_sum + nexts[0] + nexts[1])
    to_second(2)
    to_second(6)
    for n in range(2, Z):
        tables(n)
    total = of_x(0)
    z_copies[2].wait_recv()
    z_copies[6].wait_recv()
    total = total + seconds[0] + seconds[1]

    full[mine, :] = total
    sent = pl.ds(pl.multiple_of(HALF * core, 8), SHIFT)
    full_copy = remote(full.at[sent, :], full.at[sent, :], full_s, full_r, core_peer)
    full_copy.start()
    own_weights = w_buf[pl.ds(z * 2 + xl, 1), :]
    full_copy.wait()

    coeffs = full[...]
    high, low = halves(coeffs)
    scaled_high, scaled_low = halves(coeffs[0:ROWS] * own_weights)
    product = lax.dot_general(
        jnp.concatenate([scaled_high, scaled_low, scaled_high], axis=1),
        jnp.concatenate([high, high, low], axis=1),
        (((1,), (1,)), ((), ())), preferred_element_type=F32,
    )
    terms[0:21] = product[:, 0:LANES].reshape(21, 8, LANES)
    terms[21:26] = product[LANES:ROWS, LANES:256].reshape(5, 8, LANES)

    for dx, dy in PLANE[:-1]:
        j = len(plane_copies)
        xt, yt = lax.rem(x + dx, X), lax.rem(y + dy, Y)
        copy = remote(
            terms.at[(xt * Y + yt) * 2 + core], plane_in.at[j], plane_s.at[j], plane_r.at[j],
            place(xt, yt, z, core),
        )
        copy.start()
        plane_copies.append(copy)
    tile = terms[own]
    for j, copy in reversed(list(enumerate(plane_copies))):
        copy.wait_recv()
        tile = tile + plane_in[j]

    own_tile[...] = tile
    for j in (3, 2, 4, 1, 5, 0, 6):
        copy = remote(own_tile, line_in.at[j], line_s.at[j], line_r.at[j], line[j])
        copy.start()
        line_copies.append(copy)
    for j, copy in reversed(list(zip((3, 2, 4, 1, 5, 0, 6), line_copies))):
        copy.wait_recv()
        tile = tile + line_in[j]

    def to_all(buffer, send, recv):
        for j, (device, *_) in enumerate(plane):
            copy = remote(buffer.at[own], buffer.at[own], send.at[j], recv.at[j], device)
            copy.start()
            all_copies.append(copy)

    def from_all(buffer, send, recv):
        for j, (_, dx, dy, flip) in enumerate(plane):
            xs, ys = lax.rem(x + X - dx, X), lax.rem(y + Y - dy, Y)
            slot = buffer.at[(xs * Y + ys) * 2 + (core if flip == 0 else other)]
            remote(slot, slot, send.at[j], recv.at[j], core_peer).wait_recv()

    tiles[own] = tile
    to_all(tiles, all_s, all_r)
    sums[own] = contracted(tile)
    to_all(sums, sum_s, sum_r)
    from_all(tiles, all_s, all_r)
    left = tiles[0:21].reshape(ROWS, LANES)
    matrix_ref[:, 0:LANES] = left[0:CH]
    matrix_ref[0:LANES, LANES:CH] = left[LANES:ROWS].T[:, 0 : CH - LANES]
    matrix_ref[LANES:CH, LANES:CH] = tiles[21:26].reshape(40, LANES)[0 : CH - LANES, 0 : CH - LANES]
    from_all(sums, sum_s, sum_r)
    density_ref[...] = jnp.sum(sums[...], axis=0)[:, 0:HARM]
    finish()


def body(matching, vectors, weights, gaunt_index, gaunt_value):
    dma = pltpu.SemaphoreType.DMA
    depth = matching.shape[1]
    return pl.pallas_call(
        kernel,
        out_shape=(
            pltpu.VMEM((CH, CH), F32),
            pltpu.VMEM((4, HARM), F32),
        ),
        in_specs=[pl.BlockSpec(memory_space=pl.ANY)] * 5,
        out_specs=(
            pl.BlockSpec(memory_space=pltpu.VMEM),
            pl.BlockSpec(memory_space=pltpu.VMEM),
        ),
        scratch_shapes=[
            pltpu.VMEM((CH, depth), BF16),
            pltpu.VMEM((3, depth, 512), BF16),
            pltpu.VMEM((2, depth, 256), BF16),
            pltpu.VMEM((Z, 2, ROWS, LANES), F32),
            pltpu.VMEM((Z, 2, HALF, LANES), F32),
            pltpu.VMEM((Z, 2, HALF, LANES), F32),
            pltpu.VMEM((Z, HALF, LANES), F32),
            pltpu.VMEM((Z, HALF, LANES), F32),
            pltpu.VMEM((HALF, LANES), F32),
            pltpu.VMEM((2, HALF, LANES), F32),
            pltpu.VMEM((2, 2, HALF, LANES), F32),
            pltpu.VMEM((2, HALF, LANES), F32),
            pltpu.VMEM((256, LANES), F32),
            pltpu.VMEM((TILES, 8, LANES), F32),
            pltpu.VMEM((15, 8, LANES), F32),
            pltpu.VMEM((8, LANES), F32),
            pltpu.VMEM((7, 8, LANES), F32),
            pltpu.VMEM((TILES, 8, LANES), F32),
            pltpu.VMEM((16, LANES), F32),
            pltpu.VMEM((3, ENTRIES), jnp.int32),
            pltpu.VMEM((1, ENTRIES), F32),
            pltpu.VMEM((2 * LANES, ENTRIES), BF16),
            pltpu.VMEM((LANES, ENTRIES), BF16),
            pltpu.VMEM((16, ENTRIES), F32),
            pltpu.VMEM((TILES, 4, LANES), F32),
            dma, dma((Z,)), dma((3,)),
            dma((Z,)), dma((Z,)), dma((Z,)), dma((Z,)), dma((Z,)), dma((Z,)), dma, dma,
            dma((15,)), dma((15,)), dma((7,)), dma((7,)),
            dma((31,)), dma((31,)), dma((31,)), dma((31,)),
        ],
        compiler_params=pltpu.CompilerParams(
            collective_id=0, has_side_effects=True, vmem_limit_bytes=66_500_000
        ),
        name="muffin_tin",
    )(matching, vectors, weights.reshape(-1, LANES), gaunt_index, gaunt_value.reshape(1, -1))


def solution(mesh):
    return jax.shard_map(
        body,
        mesh=mesh,
        in_specs=(P(None, "basis"), P("basis", "band"), P("band"), P(), P()),
        out_specs=(P(), P()),
        check_vma=False,
    )
```

```python
import jax
import jax.numpy as jnp
from jax import lax
from jax.experimental import pallas as pl
from jax.experimental.pallas import tpu as pltpu
from jax.sharding import PartitionSpec as P

CH = 162
ROWS = 168
HALF = 88
SHIFT = 80
Z = 8
X = 4
Y = 4
LANES = 128
TILES = 32
HARM = 81
ENTRIES = 4096
CHUNK = 512
GROUPS = ((4,), (3, 5), (1, 7), (2, 6), (0,))
VIA = 48
PLANE = (
    (2, 2), (2, 1), (2, 3), (1, 2), (3, 2), (2, 0), (0, 2), (1, 1),
    (1, 3), (3, 1), (3, 3), (1, 0), (3, 0), (0, 1), (0, 3),
)
MESH = pl.DeviceIdType.MESH
F32 = jnp.float32
BF16 = jnp.bfloat16


def place(x, y, z, core):
    return {
        "basis": (z * 2 + lax.rem(x, 2)) * 2 + core,
        "band": lax.div(x, 2) * Y + y,
    }


def halves(value):
    high = value.astype(BF16)
    return high, (value - high.astype(F32)).astype(BF16)


def harmonic_of(channel):
    folded = jnp.where(channel >= HARM, channel - HARM, channel)
    return jnp.where(channel < CH, folded, -1)


def kernel(
    a_hbm, v_hbm, w_hbm, index_hbm, value_hbm, matrix_ref, density_ref,
    a_buf, v_wide, v_slim, part, core_in, pair, x_in, z_out, far, thirds, nexts, seconds,
    full, terms, plane_in,
    own_tile, line_in, tiles, w_buf, index_buf, value_buf, hot, target_hot, factor, sums, core_sums,
    a_sem, v_sem, table_sem, core_s, core_r, x_s, x_r, z_s, z_r, full_s, full_r,
    plane_s, plane_r, line_s, line_r, all_s, all_r, sum_s, sum_r, last_s, last_r,
):
    basis, band = lax.axis_index("basis"), lax.axis_index("band")
    z, xl, core = lax.div(basis, 4), lax.rem(lax.div(basis, 2), 2), lax.rem(basis, 2)
    x, y = lax.div(band, Y) * 2 + xl, lax.rem(band, Y)
    other = 1 - core
    own = core * 16 + x * Y + y

    a_copy = pltpu.make_async_copy(a_hbm, a_buf, a_sem)
    a_copy.start()
    targets = [lax.rem(z + off, Z) for off in range(Z)]
    v_blocks = (v_slim.at[0], v_wide.at[0], v_wide.at[1], v_wide.at[2], v_slim.at[1])
    v_copies = []
    for group, block in zip(GROUPS, v_blocks):
        copies = []
        for h, off in enumerate(group):
            columns = pl.ds(pl.multiple_of(targets[off] * 256, 256), 256)
            copies.append(
                pltpu.make_async_copy(
                    v_hbm.at[:, columns], block.at[:, h * 256 : h * 256 + 256], v_sem.at[off]
                )
            )
        v_copies.append(copies)
    for copy in v_copies[0] + v_copies[1]:
        copy.start()
    table_copies = [
        pltpu.make_async_copy(w_hbm, w_buf, table_sem.at[0]),
        pltpu.make_async_copy(index_hbm, index_buf, table_sem.at[1]),
        pltpu.make_async_copy(value_hbm, value_buf, table_sem.at[2]),
    ]

    plane = [
        place(lax.rem(x + dx, X), lax.rem(y + dy, Y), z, core) for dx, dy in PLANE
    ]
    core_peer = place(x, y, z, other)
    line = [place(x, y, lax.rem(z + dz, Z), core) for dz in range(1, Z)]
    barrier = pltpu.get_barrier_semaphore()
    peers = plane + line + [core_peer]
    for device in peers:
        pl.semaphore_signal(barrier, inc=1, device_id=device, device_id_type=MESH)

    for s in range(Z):
        for h in range(2):
            part[s, h, SHIFT * 2 : ROWS, :] = jnp.zeros((ROWS - SHIFT * 2, LANES), F32)
    full[ROWS:256, :] = jnp.zeros((256 - ROWS, LANES), F32)
    terms[26:TILES] = jnp.zeros((TILES - 26, 8, LANES), F32)

    x_peer = place(x + 1 - 2 * xl, y, z, core)

    def remote(src, dst, send, recv, device):
        return pltpu.make_async_remote_copy(
            src_ref=src, dst_ref=dst, send_sem=send, recv_sem=recv,
            device_id=device, device_id_type=MESH,
        )

    mine = pl.ds(pl.multiple_of(SHIFT * core, 8), HALF)
    theirs = pl.ds(pl.multiple_of(SHIFT * other, 8), HALF)
    core_copies, x_copies, z_copies = {}, {}, {}
    plane_copies, line_copies, all_copies = [], [], []

    def multiply(c):
        for copy in v_copies[c]:
            copy.wait()
        if c + 2 < len(GROUPS):
            for copy in v_copies[c + 2]:
                copy.start()
        product = jnp.dot(a_buf[...], v_blocks[c][...], preferred_element_type=F32)
        for g, off in enumerate(GROUPS[c]):
            for h in range(2):
                at = g * 256 + h * LANES
                part[off, h, 0:CH, :] = product[:, at : at + LANES]

    def to_core(off):
        core_copies[off] = remote(
            part.at[off, :, theirs, :], core_in.at[off], core_s.at[off], core_r.at[off], core_peer
        )
        core_copies[off].start()

    def of_core(off):
        core_copies[off].wait_recv()
        return part[off, :, mine, :] + core_in[off]

    def to_x(off, value):
        pair[off] = value
        x_copies[off] = remote(
            pair.at[off, 1 - xl], x_in.at[off], x_s.at[off], x_r.at[off], x_peer
        )
        x_copies[off].start()

    def of_x(off):
        x_copies[off].wait_recv()
        return pair[off, xl] + x_in[off]

    def to_z(key, src, dst, step):
        z_copies[key] = remote(
            src, dst, z_s.at[len(z_copies)], z_r.at[len(z_copies)], place(x, y, targets[step], core)
        )
        z_copies[key].start()

    def to_far():
        z_out[4] = of_x(4)
        to_z("up4", z_out.at[4, 0:VIA], far.at[0:VIA], 2)
        to_z("down4", z_out.at[4, VIA:HALF], far.at[VIA:HALF], 6)

    def to_third(off):
        z_out[off] = of_x(off)
        to_z(off, z_out.at[off], thirds.at[off // 4], 1 if off == 3 else 7)

    def to_next(off):
        pair[off] = of_core(off)
        to_z(off, pair.at[off], nexts.at[off // 4], off)

    def to_second(off):
        value = of_x(off)
        if off == 2:
            z_copies["up4"].wait_recv()
            z_copies[3].wait_recv()
            value = value + thirds[0]
            z_out[off, 0:VIA] = value[0:VIA] + far[0:VIA]
            z_out[off, VIA:HALF] = value[VIA:HALF]
        else:
            z_copies["down4"].wait_recv()
            z_copies[5].wait_recv()
            value = value + thirds[1]
            z_out[off, 0:VIA] = value[0:VIA]
            z_out[off, VIA:HALF] = value[VIA:HALF] + far[VIA:HALF]
        to_z(off, z_out.at[off], seconds.at[off // 4], off)

    first_row = own * 8 - jnp.where(own < 21, 0, 40)
    first_column = jnp.where(own < 21, 0, LANES)
    mirrored = jnp.where(jnp.logical_and(own >= 16, own < 21), 1.0, 0.0).astype(F32)
    row_channel = first_row + lax.broadcasted_iota(jnp.int32, (8, 1), 0)

    def tables(n):
        at = slice(n * CHUNK, (n + 1) * CHUNK)
        first, second = index_buf[0:1, at], index_buf[1:2, at]
        target, value = index_buf[2:3, at], value_buf[0:1, at]
        column = harmonic_of(first_column + lax.broadcasted_iota(jnp.int32, (LANES, 1), 0))
        hot[0:LANES, at] = jnp.where(column == second, 1.0, 0.0).astype(BF16)
        hot[LANES : 2 * LANES, at] = jnp.where(column == first, 1.0, 0.0).astype(BF16)
        code = lax.broadcasted_iota(jnp.int32, (LANES, 1), 0)
        target_hot[:, at] = jnp.where(code == target, 1.0, 0.0).astype(BF16)
        row = harmonic_of(row_channel)
        factor[0:8, at] = jnp.where(row == first, value, 0.0)
        factor[8:16, at] = jnp.where(row == second, value, 0.0) * mirrored

    def contracted(tile):
        lane = first_column + lax.broadcasted_iota(jnp.int32, (8, LANES), 1)
        none = jnp.zeros((8, LANES), F32)
        lows = jnp.where(lane < HARM, tile, 0.0)
        highs = jnp.where(lane < HARM, 0.0, tile)
        wide = jnp.concatenate(
            [
                jnp.concatenate([lows, highs, none, none], axis=0),
                jnp.concatenate([none, none, lows, highs], axis=0),
            ],
            axis=1,
        )
        both = jnp.concatenate(halves(wide), axis=0)
        total = jnp.zeros((8, LANES), F32)
        for n in range(ENTRIES // 1024):
            at = slice(n * 1024, (n + 1) * 1024)
            spread = jnp.dot(both, hot[:, at], preferred_element_type=F32)
            spread = spread[0:32] + spread[32:64]
            direct, mirror = factor[0:8, at], factor[8:16, at]
            low, high = spread[0:8] * direct, spread[8:16] * direct
            mirror_low, mirror_high = spread[16:24] * mirror, spread[24:32] * mirror
            upper = row_channel >= HARM
            rows = [
                jnp.where(upper, 0.0, low),
                jnp.where(upper, 0.0, high) + mirror_low,
                jnp.where(upper, low, 0.0),
                jnp.where(upper, high, 0.0) + mirror_high,
            ]
            values = jnp.concatenate([jnp.sum(row, axis=0, keepdims=True) for row in rows], axis=0)
            total = total + lax.dot_general(
                jnp.concatenate(halves(values), axis=0), target_hot[:, at],
                (((1,), (1,)), ((), ())), preferred_element_type=F32,
            )
        return total[0:4] + total[4:8]

    def finish():
        for copies in (core_copies, x_copies, z_copies):
            for copy in copies.values():
                copy.wait_send()
        for copy in plane_copies + line_copies + all_copies:
            copy.wait_send()

    a_copy.wait()
    multiply(0)
    pl.semaphore_wait(barrier, len(peers))
    to_core(4)
    for copy in table_copies:
        copy.start()
    multiply(1)
    to_core(3)
    to_core(5)
    to_x(4, of_core(4))
    multiply(2)
    to_core(1)
    to_core(7)
    to_x(3, of_core(3))
    to_x(5, of_core(5))
    multiply(3)
    to_core(2)
    to_core(6)
    to_next(1)
    to_next(7)
    multiply(4)
    to_core(0)
    to_far()
    to_x(2, of_core(2))
    to_x(6, of_core(6))
    to_third(3)
    to_third(5)
    own_sum = of_core(0)
    for copy in table_copies:
        copy.wait()
    for n in range(2):
        tables(n)
    z_copies[1].wait_recv()
    z_copies[7].wait_recv()
    to_x(0, own_sum + nexts[0] + nexts[1])
    to_second(2)
    to_second(6)
    for n in range(2, Z):
        tables(n)
    total = of_x(0)
    z_copies[2].wait_recv()
    z_copies[6].wait_recv()
    total = total + seconds[0] + seconds[1]

    full[mine, :] = total
    sent = pl.ds(pl.multiple_of(HALF * core, 8), SHIFT)
    full_copy = remote(full.at[sent, :], full.at[sent, :], full_s, full_r, core_peer)
    full_copy.start()
    own_weights = w_buf[pl.ds(z * 2 + xl, 1), :]
    full_copy.wait()

    coeffs = full[...]
    high, low = halves(coeffs)
    scaled_high, scaled_low = halves(coeffs[0:ROWS] * own_weights)
    product = lax.dot_general(
        jnp.concatenate([scaled_high, scaled_low, scaled_high], axis=1),
        jnp.concatenate([high, high, low], axis=1),
        (((1,), (1,)), ((), ())), preferred_element_type=F32,
    )
    terms[0:21] = product[:, 0:LANES].reshape(21, 8, LANES)
    terms[21:26] = product[LANES:ROWS, LANES:256].reshape(5, 8, LANES)

    for j, (dx, dy) in enumerate(PLANE):
        target = core * 16 + lax.rem(x + dx, X) * Y + lax.rem(y + dy, Y)
        copy = remote(terms.at[target], plane_in.at[j], plane_s.at[j], plane_r.at[j], plane[j])
        copy.start()
        plane_copies.append(copy)
    tile = terms[own]
    for j, copy in reversed(list(enumerate(plane_copies))):
        copy.wait_recv()
        tile = tile + plane_in[j]

    own_tile[...] = tile
    for j in (3, 2, 4, 1, 5, 0, 6):
        copy = remote(own_tile, line_in.at[j], line_s.at[j], line_r.at[j], line[j])
        copy.start()
        line_copies.append(copy)
    for j, copy in reversed(list(zip((3, 2, 4, 1, 5, 0, 6), line_copies))):
        copy.wait_recv()
        tile = tile + line_in[j]

    def to_all(buffer, send, recv):
        for j, device in enumerate(plane):
            all_copies.append(remote(buffer.at[own], buffer.at[own], send.at[j], recv.at[j], device))
            all_copies[-1].start()

    def from_all(buffer, send, recv):
        for j, (dx, dy) in reversed(list(enumerate(PLANE))):
            slot = buffer.at[
                core * 16 + lax.rem(x + X - dx, X) * Y + lax.rem(y + Y - dy, Y)
            ]
            remote(slot, slot, send.at[j], recv.at[j], core_peer).wait_recv()

    def to_core_peer(ref, k):
        all_copies.append(remote(ref, ref, last_s.at[k], last_r.at[k], core_peer))
        all_copies[-1].start()
        return all_copies[-1]

    tiles[own] = tile
    to_all(tiles, all_s, all_r)
    sums[own] = contracted(tile)
    to_all(sums, sum_s, sum_r)
    from_all(tiles, all_s, all_r)
    own_half = pl.ds(pl.multiple_of(16 * core, 16), 16)
    tiles_copy = to_core_peer(tiles.at[own_half], 0)
    from_all(sums, sum_s, sum_r)
    core_sums[core] = jnp.sum(sums[own_half], axis=0)
    sums_copy = to_core_peer(core_sums.at[core], 1)
    tiles_copy.wait_recv()
    left = tiles[0:21].reshape(ROWS, LANES)
    matrix_ref[:, 0:LANES] = left[0:CH]
    matrix_ref[0:LANES, LANES:CH] = left[LANES:ROWS].T[:, 0 : CH - LANES]
    matrix_ref[LANES:CH, LANES:CH] = tiles[21:26].reshape(40, LANES)[0 : CH - LANES, 0 : CH - LANES]
    sums_copy.wait_recv()
    density_ref[...] = (core_sums[0] + core_sums[1])[:, 0:HARM]
    finish()


def body(matching, vectors, weights, gaunt_index, gaunt_value):
    dma = pltpu.SemaphoreType.DMA
    depth = matching.shape[1]
    return pl.pallas_call(
        kernel,
        out_shape=(
            pltpu.VMEM((CH, CH), F32),
            pltpu.VMEM((4, HARM), F32),
        ),
        in_specs=[pl.BlockSpec(memory_space=pl.ANY)] * 5,
        out_specs=(
            pl.BlockSpec(memory_space=pltpu.VMEM),
            pl.BlockSpec(memory_space=pltpu.VMEM),
        ),
        scratch_shapes=[
            pltpu.VMEM((CH, depth), BF16),
            pltpu.VMEM((3, depth, 512), BF16),
            pltpu.VMEM((2, depth, 256), BF16),
            pltpu.VMEM((Z, 2, ROWS, LANES), F32),
            pltpu.VMEM((Z, 2, HALF, LANES), F32),
            pltpu.VMEM((Z, 2, HALF, LANES), F32),
            pltpu.VMEM((Z, HALF, LANES), F32),
            pltpu.VMEM((Z, HALF, LANES), F32),
            pltpu.VMEM((HALF, LANES), F32),
            pltpu.VMEM((2, HALF, LANES), F32),
            pltpu.VMEM((2, 2, HALF, LANES), F32),
            pltpu.VMEM((2, HALF, LANES), F32),
            pltpu.VMEM((256, LANES), F32),
            pltpu.VMEM((TILES, 8, LANES), F32),
            pltpu.VMEM((15, 8, LANES), F32),
            pltpu.VMEM((8, LANES), F32),
            pltpu.VMEM((7, 8, LANES), F32),
            pltpu.VMEM((TILES, 8, LANES), F32),
            pltpu.VMEM((16, LANES), F32),
            pltpu.VMEM((3, ENTRIES), jnp.int32),
            pltpu.VMEM((1, ENTRIES), F32),
            pltpu.VMEM((2 * LANES, ENTRIES), BF16),
            pltpu.VMEM((LANES, ENTRIES), BF16),
            pltpu.VMEM((16, ENTRIES), F32),
            pltpu.VMEM((TILES, 4, LANES), F32),
            pltpu.VMEM((2, 4, LANES), F32),
            dma, dma((Z,)), dma((3,)),
            dma((Z,)), dma((Z,)), dma((Z,)), dma((Z,)), dma((Z,)), dma((Z,)), dma, dma,
            dma((15,)), dma((15,)), dma((7,)), dma((7,)),
            dma((15,)), dma((15,)), dma((15,)), dma((15,)), dma((2,)), dma((2,)),
        ],
        compiler_params=pltpu.CompilerParams(
            collective_id=0, has_side_effects=True, vmem_limit_bytes=66_500_000
        ),
        name="muffin_tin",
    )(matching, vectors, weights.reshape(-1, LANES), gaunt_index, gaunt_value.reshape(1, -1))


def solution(mesh):
    return jax.shard_map(
        body,
        mesh=mesh,
        in_specs=(P(None, "basis"), P("basis", "band"), P("band"), P(), P()),
        out_specs=(P(), P()),
        check_vma=False,
    )
```

```python
import jax
import jax.numpy as jnp
from jax import lax
from jax.experimental import pallas as pl
from jax.experimental.pallas import tpu as pltpu
from jax.sharding import PartitionSpec as P

CH = 162
ROWS = 168
HALF = 88
SHIFT = 80
Z = 8
X = 4
Y = 4
LANES = 128
TILES = 32
HARM = 81
ENTRIES = 4096
CHUNK = 512
GROUPS = ((4,), (3, 5), (1, 7), (2, 6), (0,))
VIA = 48
PLANE = (
    (2, 2), (2, 1), (2, 3), (1, 2), (3, 2), (2, 0), (0, 2), (1, 1),
    (1, 3), (3, 1), (3, 3), (1, 0), (3, 0), (0, 1), (0, 3),
)
MESH = pl.DeviceIdType.MESH
F32 = jnp.float32
BF16 = jnp.bfloat16


def place(x, y, z, core):
    return {
        "basis": (z * 2 + lax.rem(x, 2)) * 2 + core,
        "band": lax.div(x, 2) * Y + y,
    }


def halves(value):
    high = value.astype(BF16)
    return high, (value - high.astype(F32)).astype(BF16)


def harmonic_of(channel):
    folded = jnp.where(channel >= HARM, channel - HARM, channel)
    return jnp.where(channel < CH, folded, -1)


def kernel(
    a_hbm, v_hbm, w_hbm, index_hbm, value_hbm, matrix_ref, density_ref,
    a_buf, v_wide, v_slim, part, core_in, pair, x_in, z_out, far, thirds, nexts, seconds,
    full, terms, plane_in,
    own_tile, line_in, tiles, w_buf, index_buf, value_buf, hot, target_hot, factor, sums, core_sums,
    a_sem, v_sem, table_sem, core_s, core_r, x_s, x_r, z_s, z_r, full_s, full_r,
    plane_s, plane_r, line_s, line_r, all_s, all_r, sum_s, sum_r, last_s, last_r,
):
    basis, band = lax.axis_index("basis"), lax.axis_index("band")
    z, xl, core = lax.div(basis, 4), lax.rem(lax.div(basis, 2), 2), lax.rem(basis, 2)
    x, y = lax.div(band, Y) * 2 + xl, lax.rem(band, Y)
    other = 1 - core
    own = core * 16 + x * Y + y

    a_copy = pltpu.make_async_copy(a_hbm, a_buf, a_sem)
    a_copy.start()
    targets = [lax.rem(z + off, Z) for off in range(Z)]
    v_blocks = (v_slim.at[0], v_wide.at[0], v_wide.at[1], v_wide.at[2], v_slim.at[1])
    v_copies = []
    for group, block in zip(GROUPS, v_blocks):
        copies = []
        for h, off in enumerate(group):
            columns = pl.ds(pl.multiple_of(targets[off] * 256, 256), 256)
            copies.append(
                pltpu.make_async_copy(
                    v_hbm.at[:, columns], block.at[:, h * 256 : h * 256 + 256], v_sem.at[off]
                )
            )
        v_copies.append(copies)
    for copy in v_copies[0] + v_copies[1] + v_copies[2]:
        copy.start()
    table_copies = [
        pltpu.make_async_copy(w_hbm, w_buf, table_sem.at[0]),
        pltpu.make_async_copy(index_hbm, index_buf, table_sem.at[1]),
        pltpu.make_async_copy(value_hbm, value_buf, table_sem.at[2]),
    ]

    plane = [
        place(lax.rem(x + dx, X), lax.rem(y + dy, Y), z, core) for dx, dy in PLANE
    ]
    core_peer = place(x, y, z, other)
    line = [place(x, y, lax.rem(z + dz, Z), core) for dz in range(1, Z)]
    barrier = pltpu.get_barrier_semaphore()
    peers = plane + line + [core_peer]
    for device in peers:
        pl.semaphore_signal(barrier, inc=1, device_id=device, device_id_type=MESH)

    for s in range(Z):
        for h in range(2):
            part[s, h, SHIFT * 2 : ROWS, :] = jnp.zeros((ROWS - SHIFT * 2, LANES), F32)
    full[ROWS:256, :] = jnp.zeros((256 - ROWS, LANES), F32)
    terms[26:TILES] = jnp.zeros((TILES - 26, 8, LANES), F32)

    x_peer = place(x + 1 - 2 * xl, y, z, core)

    def remote(src, dst, send, recv, device):
        return pltpu.make_async_remote_copy(
            src_ref=src, dst_ref=dst, send_sem=send, recv_sem=recv,
            device_id=device, device_id_type=MESH,
        )

    mine = pl.ds(pl.multiple_of(SHIFT * core, 8), HALF)
    theirs = pl.ds(pl.multiple_of(SHIFT * other, 8), HALF)
    core_copies, x_copies, z_copies = {}, {}, {}
    plane_copies, line_copies, all_copies = [], [], []

    def multiply(c):
        for copy in v_copies[c]:
            copy.wait()
        if c + 3 < len(GROUPS):
            for copy in v_copies[c + 3]:
                copy.start()
        product = jnp.dot(a_buf[...], v_blocks[c][...], preferred_element_type=F32)
        for g, off in enumerate(GROUPS[c]):
            for h in range(2):
                at = g * 256 + h * LANES
                part[off, h, 0:CH, :] = product[:, at : at + LANES]

    def to_core(off):
        core_copies[off] = remote(
            part.at[off, :, theirs, :], core_in.at[off], core_s.at[off], core_r.at[off], core_peer
        )
        core_copies[off].start()

    def of_core(off):
        core_copies[off].wait_recv()
        return part[off, :, mine, :] + core_in[off]

    def to_x(off, value):
        pair[off] = value
        x_copies[off] = remote(
            pair.at[off, 1 - xl], x_in.at[off], x_s.at[off], x_r.at[off], x_peer
        )
        x_copies[off].start()

    def of_x(off):
        x_copies[off].wait_recv()
        return pair[off, xl] + x_in[off]

    def to_z(key, src, dst, step):
        z_copies[key] = remote(
            src, dst, z_s.at[len(z_copies)], z_r.at[len(z_copies)], place(x, y, targets[step], core)
        )
        z_copies[key].start()

    def to_far():
        z_out[4] = of_x(4)
        to_z("up4", z_out.at[4, 0:VIA], far.at[0:VIA], 2)
        to_z("down4", z_out.at[4, VIA:HALF], far.at[VIA:HALF], 6)

    def to_third(off):
        z_out[off] = of_x(off)
        to_z(off, z_out.at[off], thirds.at[off // 4], 1 if off == 3 else 7)

    def to_next(off):
        pair[off] = of_core(off)
        to_z(off, pair.at[off], nexts.at[off // 4], off)

    def to_second(off):
        value = of_x(off)
        if off == 2:
            z_copies["up4"].wait_recv()
            z_copies[3].wait_recv()
            value = value + thirds[0]
            z_out[off, 0:VIA] = value[0:VIA] + far[0:VIA]
            z_out[off, VIA:HALF] = value[VIA:HALF]
        else:
            z_copies["down4"].wait_recv()
            z_copies[5].wait_recv()
            value = value + thirds[1]
            z_out[off, 0:VIA] = value[0:VIA]
            z_out[off, VIA:HALF] = value[VIA:HALF] + far[VIA:HALF]
        to_z(off, z_out.at[off], seconds.at[off // 4], off)

    first_row = own * 8 - jnp.where(own < 21, 0, 40)
    first_column = jnp.where(own < 21, 0, LANES)
    mirrored = jnp.where(jnp.logical_and(own >= 16, own < 21), 1.0, 0.0).astype(F32)
    row_channel = first_row + lax.broadcasted_iota(jnp.int32, (8, 1), 0)

    def tables(n):
        at = slice(n * CHUNK, (n + 1) * CHUNK)
        first, second = index_buf[0:1, at], index_buf[1:2, at]
        target, value = index_buf[2:3, at], value_buf[0:1, at]
        column = harmonic_of(first_column + lax.broadcasted_iota(jnp.int32, (LANES, 1), 0))
        hot[0:LANES, at] = jnp.where(column == second, 1.0, 0.0).astype(BF16)
        hot[LANES : 2 * LANES, at] = jnp.where(column == first, 1.0, 0.0).astype(BF16)
        code = lax.broadcasted_iota(jnp.int32, (LANES, 1), 0)
        target_hot[:, at] = jnp.where(code == target, 1.0, 0.0).astype(BF16)
        row = harmonic_of(row_channel)
        factor[0:8, at] = jnp.where(row == first, value, 0.0)
        factor[8:16, at] = jnp.where(row == second, value, 0.0) * mirrored

    def contracted(tile):
        lane = first_column + lax.broadcasted_iota(jnp.int32, (8, LANES), 1)
        none = jnp.zeros((8, LANES), F32)
        lows = jnp.where(lane < HARM, tile, 0.0)
        highs = jnp.where(lane < HARM, 0.0, tile)
        wide = jnp.concatenate(
            [
                jnp.concatenate([lows, highs, none, none], axis=0),
                jnp.concatenate([none, none, lows, highs], axis=0),
            ],
            axis=1,
        )
        both = jnp.concatenate(halves(wide), axis=0)
        total = jnp.zeros((8, LANES), F32)
        for n in range(ENTRIES // 1024):
            at = slice(n * 1024, (n + 1) * 1024)
            spread = jnp.dot(both, hot[:, at], preferred_element_type=F32)
            spread = spread[0:32] + spread[32:64]
            direct, mirror = factor[0:8, at], factor[8:16, at]
            low, high = spread[0:8] * direct, spread[8:16] * direct
            mirror_low, mirror_high = spread[16:24] * mirror, spread[24:32] * mirror
            upper = row_channel >= HARM
            rows = [
                jnp.where(upper, 0.0, low),
                jnp.where(upper, 0.0, high) + mirror_low,
                jnp.where(upper, low, 0.0),
                jnp.where(upper, high, 0.0) + mirror_high,
            ]
            values = jnp.concatenate([jnp.sum(row, axis=0, keepdims=True) for row in rows], axis=0)
            total = total + lax.dot_general(
                jnp.concatenate(halves(values), axis=0), target_hot[:, at],
                (((1,), (1,)), ((), ())), preferred_element_type=F32,
            )
        return total[0:4] + total[4:8]

    def finish():
        for copies in (core_copies, x_copies, z_copies):
            for copy in copies.values():
                copy.wait_send()
        for copy in plane_copies + line_copies + all_copies:
            copy.wait_send()

    a_copy.wait()
    multiply(0)
    pl.semaphore_wait(barrier, len(peers))
    to_core(4)
    for copy in table_copies:
        copy.start()
    multiply(1)
    to_core(3)
    to_core(5)
    to_x(4, of_core(4))
    multiply(2)
    to_core(1)
    to_core(7)
    to_x(5, of_core(5))
    to_x(3, of_core(3))
    multiply(3)
    to_core(2)
    to_core(6)
    to_next(1)
    to_next(7)
    multiply(4)
    to_core(0)
    to_far()
    to_x(2, of_core(2))
    to_x(6, of_core(6))
    to_third(3)
    to_third(5)
    own_sum = of_core(0)
    for copy in table_copies:
        copy.wait()
    for n in range(2):
        tables(n)
    z_copies[1].wait_recv()
    z_copies[7].wait_recv()
    to_x(0, own_sum + nexts[0] + nexts[1])
    to_second(2)
    to_second(6)
    for n in range(2, Z):
        tables(n)
    total = of_x(0)
    z_copies[2].wait_recv()
    z_copies[6].wait_recv()
    total = total + seconds[0] + seconds[1]

    full[mine, :] = total
    sent = pl.ds(pl.multiple_of(HALF * core, 8), SHIFT)
    full_copy = remote(full.at[sent, :], full.at[sent, :], full_s, full_r, core_peer)
    full_copy.start()
    own_weights = w_buf[pl.ds(z * 2 + xl, 1), :]
    full_copy.wait()

    coeffs = full[...]
    high, low = halves(coeffs)
    scaled_high, scaled_low = halves(coeffs[0:ROWS] * own_weights)
    product = lax.dot_general(
        jnp.concatenate([scaled_high, scaled_low, scaled_high], axis=1),
        jnp.concatenate([high, high, low], axis=1),
        (((1,), (1,)), ((), ())), preferred_element_type=F32,
    )
    terms[0:21] = product[:, 0:LANES].reshape(21, 8, LANES)
    terms[21:26] = product[LANES:ROWS, LANES:256].reshape(5, 8, LANES)

    for j, (dx, dy) in enumerate(PLANE):
        target = core * 16 + lax.rem(x + dx, X) * Y + lax.rem(y + dy, Y)
        copy = remote(terms.at[target], plane_in.at[j], plane_s.at[j], plane_r.at[j], plane[j])
        copy.start()
        plane_copies.append(copy)
    tile = terms[own]
    for j, copy in reversed(list(enumerate(plane_copies))):
        copy.wait_recv()
        tile = tile + plane_in[j]

    own_tile[...] = tile
    for j in (3, 2, 4, 1, 5, 0, 6):
        copy = remote(own_tile, line_in.at[j], line_s.at[j], line_r.at[j], line[j])
        copy.start()
        line_copies.append(copy)
    for j, copy in reversed(list(zip((3, 2, 4, 1, 5, 0, 6), line_copies))):
        copy.wait_recv()
        tile = tile + line_in[j]

    def to_all(buffer, send, recv):
        for j, device in enumerate(plane):
            all_copies.append(remote(buffer.at[own], buffer.at[own], send.at[j], recv.at[j], device))
            all_copies[-1].start()

    def from_all(buffer, send, recv):
        for j, (dx, dy) in reversed(list(enumerate(PLANE))):
            slot = buffer.at[
                core * 16 + lax.rem(x + X - dx, X) * Y + lax.rem(y + Y - dy, Y)
            ]
            remote(slot, slot, send.at[j], recv.at[j], core_peer).wait_recv()

    def to_core_peer(ref, k):
        all_copies.append(remote(ref, ref, last_s.at[k], last_r.at[k], core_peer))
        all_copies[-1].start()
        return all_copies[-1]

    tiles[own] = tile
    to_all(tiles, all_s, all_r)
    sums[own] = contracted(tile)
    to_all(sums, sum_s, sum_r)
    from_all(tiles, all_s, all_r)
    own_half = pl.ds(pl.multiple_of(16 * core, 16), 16)
    tiles_copy = to_core_peer(tiles.at[own_half], 0)
    from_all(sums, sum_s, sum_r)
    core_sums[core] = jnp.sum(sums[own_half], axis=0)
    sums_copy = to_core_peer(core_sums.at[core], 1)
    tiles_copy.wait_recv()
    left = tiles[0:21].reshape(ROWS, LANES)
    matrix_ref[:, 0:LANES] = left[0:CH]
    matrix_ref[0:LANES, LANES:CH] = left[LANES:ROWS].T[:, 0 : CH - LANES]
    matrix_ref[LANES:CH, LANES:CH] = tiles[21:26].reshape(40, LANES)[0 : CH - LANES, 0 : CH - LANES]
    sums_copy.wait_recv()
    density_ref[...] = (core_sums[0] + core_sums[1])[:, 0:HARM]
    finish()


def body(matching, vectors, weights, gaunt_index, gaunt_value):
    dma = pltpu.SemaphoreType.DMA
    depth = matching.shape[1]
    return pl.pallas_call(
        kernel,
        out_shape=(
            pltpu.VMEM((CH, CH), F32),
            pltpu.VMEM((4, HARM), F32),
        ),
        in_specs=[pl.BlockSpec(memory_space=pl.ANY)] * 5,
        out_specs=(
            pl.BlockSpec(memory_space=pltpu.VMEM),
            pl.BlockSpec(memory_space=pltpu.VMEM),
        ),
        scratch_shapes=[
            pltpu.VMEM((CH, depth), BF16),
            pltpu.VMEM((3, depth, 512), BF16),
            pltpu.VMEM((2, depth, 256), BF16),
            pltpu.VMEM((Z, 2, ROWS, LANES), F32),
            pltpu.VMEM((Z, 2, HALF, LANES), F32),
            pltpu.VMEM((Z, 2, HALF, LANES), F32),
            pltpu.VMEM((Z, HALF, LANES), F32),
            pltpu.VMEM((Z, HALF, LANES), F32),
            pltpu.VMEM((HALF, LANES), F32),
            pltpu.VMEM((2, HALF, LANES), F32),
            pltpu.VMEM((2, 2, HALF, LANES), F32),
            pltpu.VMEM((2, HALF, LANES), F32),
            pltpu.VMEM((256, LANES), F32),
            pltpu.VMEM((TILES, 8, LANES), F32),
            pltpu.VMEM((15, 8, LANES), F32),
            pltpu.VMEM((8, LANES), F32),
            pltpu.VMEM((7, 8, LANES), F32),
            pltpu.VMEM((TILES, 8, LANES), F32),
            pltpu.VMEM((16, LANES), F32),
            pltpu.VMEM((3, ENTRIES), jnp.int32),
            pltpu.VMEM((1, ENTRIES), F32),
            pltpu.VMEM((2 * LANES, ENTRIES), BF16),
            pltpu.VMEM((LANES, ENTRIES), BF16),
            pltpu.VMEM((16, ENTRIES), F32),
            pltpu.VMEM((TILES, 4, LANES), F32),
            pltpu.VMEM((2, 4, LANES), F32),
            dma, dma((Z,)), dma((3,)),
            dma((Z,)), dma((Z,)), dma((Z,)), dma((Z,)), dma((Z,)), dma((Z,)), dma, dma,
            dma((15,)), dma((15,)), dma((7,)), dma((7,)),
            dma((15,)), dma((15,)), dma((15,)), dma((15,)), dma((2,)), dma((2,)),
        ],
        compiler_params=pltpu.CompilerParams(
            collective_id=0, has_side_effects=True, vmem_limit_bytes=66_500_000
        ),
        name="muffin_tin",
    )(matching, vectors, weights.reshape(-1, LANES), gaunt_index, gaunt_value.reshape(1, -1))


def solution(mesh):
    return jax.shard_map(
        body,
        mesh=mesh,
        in_specs=(P(None, "basis"), P("basis", "band"), P("band"), P(), P()),
        out_specs=(P(), P()),
        check_vma=False,
    )
```
